32 devices in a mesh: blk: 16 (over z, y, x), grp: 2 (over core).
Axes of the slice: x: 2, y: 2, z: 4, core: 2. Of those that a mesh axis runs over, the one named last changes fastest.
Arguments:
- text: bfloat16 [16, 384, 1024], P('blk', 'grp'), may hold values from -64 to 64
- image: bfloat16 [16, 384, 1024], P('blk', 'grp'), may hold values from -64 to 64
- pair_index: int32 [16, 384], P('blk', 'grp'), may hold values from 0 to 383, each once within a row
Outputs:
- grad_text: float32 [16, 384, 1024], P('blk', 'grp')
- grad_image: float32 [16, 384, 1024], P('blk', 'grp')
- loss: float32 [], replicated
The draws below stay inside these ranges and needn't reach their ends.
Inputs may be any that keep to these rules, and one draw needn't show every extreme that they name: Every sub-batch's row of pair_index names each of 0 to 383 once.
All inputs are finite; a program needn't handle non-finite values.
Results may differ from the reference program's by a relative error of at most 0.0024.
Values may be sent and summed in bfloat16 or wider, within the bound.
No kernel may reach another device: no remote copies, remote signals or barrier semaphores. Data moves between devices by JAX's collectives and lax.ppermute only.
A program may use at most 64 MiB of HBM per device.

```python
import jax
import jax.numpy as jnp

D = 1024
SUB = 384
GROUPS = 16


def embed_pair(key):
    key = jax.random.fold_in(key, 7)
    keys = jax.random.split(key, 6)
    text_base = jax.random.normal(keys[0], (GROUPS, SUB, D), jnp.float32)
    image_base = jax.random.normal(keys[1], (GROUPS, SUB, D), jnp.float32)
    text_out = text_base
    image_out = image_base
    targets = (110.0, 150.0, 200.0, 260.0)
    for number in range(4):
        target = targets[number]
        first_row = number * (SUB // 4)
        base = image_base[:, first_row + 1]
        noise_a = jax.random.normal(jax.random.fold_in(keys[4], number), (GROUPS, D), jnp.float32)
        noise_b = jax.random.normal(jax.random.fold_in(keys[5], number), (GROUPS, D), jnp.float32)
        base_sq = jnp.sum(base * base, axis=-1, keepdims=True)
        perp_a = noise_a - jnp.sum(noise_a * base, axis=-1, keepdims=True) / base_sq * base
        perp_b = noise_b - jnp.sum(noise_b * base, axis=-1, keepdims=True) / base_sq * base
        stretch = jnp.sqrt(target / (0.125 * base_sq))
        aligned = stretch * base
        shrink = 1.0 - 2.0 / target
        image_out = image_out.at[:, first_row + 1].set(aligned)
        image_out = image_out.at[:, first_row + 2].set(shrink * aligned + perp_a)
        text_out = text_out.at[:, first_row].set(aligned)
        text_out = text_out.at[:, first_row + 1].set(shrink * aligned + perp_b)
    return (jnp.clip(text_out, -64.0, 64.0), jnp.clip(image_out, -64.0, 64.0))


def draw_text(key, part):
    return embed_pair(key)[0].astype(jnp.bfloat16)


def draw_image(key, part):
    return embed_pair(key)[1].astype(jnp.bfloat16)


def setup_inputs(seed: int = 0) -> dict:
    key_of = jax.random.split(jax.random.key(seed), 4)
    return {
        "text": draw_text(jax.random.fold_in(key_of[3], 71), 0),
        "image": draw_image(jax.random.fold_in(key_of[3], 71), 0),
        "pair_index": jax.vmap(lambda own: jax.random.permutation(own, SUB))(jax.random.split(key_of[2], GROUPS)).reshape((GROUPS, SUB)).astype(jnp.int32),
    }


score_scale = 0.125


def group_terms(text_rows, image_rows, pairs):
    scores = jnp.dot(text_rows, image_rows.T, preferred_element_type=jnp.float32) * score_scale
    row_top = jnp.max(scores, axis=1)
    row_lse = row_top + jnp.log(jnp.sum(jnp.exp(scores - row_top[:, None]), axis=1))
    col_top = jnp.max(scores, axis=0)
    col_lse = col_top + jnp.log(jnp.sum(jnp.exp(scores - col_top[None, :]), axis=0))
    hit = pairs[:, None] == jnp.arange(SUB, dtype=jnp.int32)[None, :]
    positive = jnp.sum(jnp.where(hit, scores, 0.0), axis=1)
    weight = (jnp.exp(scores - row_lse[:, None]) + jnp.exp(scores - col_lse[None, :]) - 2.0 * hit.astype(jnp.float32)).astype(jnp.bfloat16)
    grad_t = jnp.dot(weight, image_rows, preferred_element_type=jnp.float32) * (score_scale * 0.5)
    grad_i = jnp.dot(weight.T, text_rows, preferred_element_type=jnp.float32) * (score_scale * 0.5)
    partial_sum = jnp.sum(row_lse - 2.0 * positive) + jnp.sum(col_lse)
    return grad_t, grad_i, partial_sum


def reference(text, image, pair_index):
    grads_t = []
    grads_i = []
    total = jnp.zeros((), jnp.float32)
    for group in range(GROUPS):
        grad_t, grad_i, partial_sum = group_terms(text[group], image[group], pair_index[group])
        grads_t.append(grad_t)
        grads_i.append(grad_i)
        total = total + partial_sum
    loss = total / (2.0 * SUB * GROUPS)
    return jnp.stack(grads_t), jnp.stack(grads_i), loss
```

```python
import functools

import jax
import jax.numpy as jnp
from jax import lax
from jax.experimental import pallas as pl
from jax.experimental.pallas import tpu as pltpu
from jax.sharding import PartitionSpec as P

score_scale = 0.125
BOTH = ("blk", "grp")


def in_order(me, count, pieces, body):
    for member in range(count):

        @pl.when(me == member)
        def _():
            body([pieces[(owner - member) % count] for owner in range(count)])


def joined(refs):
    return jnp.concatenate([ref[...] for ref in refs], axis=0)


def column_of(row):
    n = row.shape[1]
    eye = lax.broadcasted_iota(jnp.int32, (n, n), 0) == lax.broadcasted_iota(jnp.int32, (n, n), 1)
    spread = jnp.where(eye, jnp.broadcast_to(row, (n, n)), 0.0)
    return jnp.sum(spread, axis=1, keepdims=True)


def stats_kernel(count, *refs):
    texts, images, pairs = refs[:count], refs[count : 2 * count], refs[2 * count : 3 * count]
    scores_ref, row_ref, col_ref, pair_ref, part_ref = refs[3 * count :]
    me = lax.axis_index("grp")
    rows = pairs[0].shape[1]
    total = rows * count

    for k in range(count):
        owner = lax.rem(me + k, count)
        at = pl.ds(pl.multiple_of(owner * rows, rows), rows)
        pair_ref[at, :] = column_of(pairs[k][...].astype(jnp.float32)).astype(jnp.int32)

    def score(ordered):
        scores_ref[...] = (
            lax.dot_general(
                joined([t for t, _ in ordered]),
                joined([i for _, i in ordered]),
                (((1,), (1,)), ((), ())),
                preferred_element_type=jnp.float32,
            )
            * score_scale
        )

    in_order(me, count, list(zip(texts, images)), score)
    scores = scores_ref[...]
    row_top = jnp.max(scores, axis=1, keepdims=True)
    col_top = jnp.max(scores, axis=0, keepdims=True)
    row_lse = row_top + jnp.log(jnp.sum(jnp.exp(scores - row_top), axis=1, keepdims=True))
    col_lse = col_top + jnp.log(jnp.sum(jnp.exp(scores - col_top), axis=0, keepdims=True))
    row_ref[...] = row_lse
    col_ref[...] = col_lse
    ids = lax.broadcasted_iota(jnp.int32, (total, total), 1)
    hits = jnp.where(pair_ref[...] == ids, scores, 0.0)
    positive = jnp.sum(jnp.sum(hits, axis=0, keepdims=True), axis=1, keepdims=True)
    part = (
        jnp.sum(row_lse, axis=0, keepdims=True)
        + jnp.sum(col_lse, axis=1, keepdims=True)
        - 2.0 * positive
    )
    part_ref[...] = jnp.broadcast_to(part, part_ref.shape)


def weight_of(scores, row_lse, col_lse, pairs, ids):
    hit = jnp.where(pairs == ids, 2.0, 0.0)
    return (jnp.exp(scores - row_lse) + jnp.exp(scores - col_lse) - hit).astype(jnp.bfloat16)


def text_kernel(count, *refs):
    images = refs[:count]
    scores_ref, row_ref, col_ref, pair_ref, out_ref = refs[count:]
    me = lax.axis_index("grp")
    rows = out_ref.shape[0]
    at = pl.ds(pl.multiple_of(me * rows, rows), rows)
    ids = lax.broadcasted_iota(jnp.int32, (rows, rows * count), 1)
    weight = weight_of(scores_ref[at, :], row_ref[at, :], col_ref[...], pair_ref[at, :], ids)

    def multiply(ordered):
        out_ref[...] = jnp.dot(
            weight, joined(ordered), preferred_element_type=jnp.float32
        ) * (score_scale * 0.5)

    in_order(me, count, images, multiply)


def image_kernel(count, *refs):
    texts = refs[:count]
    scores_ref, row_ref, col_ref, pair_ref, out_ref = refs[count:]
    me = lax.axis_index("grp")
    rows = out_ref.shape[0]
    for member in range(count):

        @pl.when(me == member)
        def _():
            at = slice(member * rows, (member + 1) * rows)
            ids = lax.broadcasted_iota(jnp.int32, (rows * count, rows), 1) + member * rows
            weight = weight_of(
                scores_ref[:, at], row_ref[...], col_ref[:, at], pair_ref[...], ids
            )
            ordered = [texts[(owner - member) % count] for owner in range(count)]
            out_ref[...] = lax.dot_general(
                weight,
                joined(ordered),
                (((0,), (0,)), ((), ())),
                preferred_element_type=jnp.float32,
            ) * (score_scale * 0.5)


def in_vmem(n):
    return [pl.BlockSpec(memory_space=pltpu.VMEM)] * n


def local(text, image, pair_index):
    count = lax.axis_size("grp")
    blocks = lax.axis_size("blk")
    rows, width = text.shape[1:]
    total = rows * count

    def members(value):
        steps = range(1, count)
        turned = [
            lax.ppermute(value, "grp", [(i, (i - k) % count) for i in range(count)])
            for k in steps
        ]
        return [value, *turned]

    images = members(image[0])
    texts = members(text[0])
    pairs = members(pair_index)

    scores, row_lse, col_lse, pair_column, part = pl.pallas_call(
        functools.partial(stats_kernel, count),
        out_shape=(
            jax.ShapeDtypeStruct((total, total), jnp.float32),
            jax.ShapeDtypeStruct((total, 1), jnp.float32),
            jax.ShapeDtypeStruct((1, total), jnp.float32),
            jax.ShapeDtypeStruct((total, 1), jnp.int32),
            jax.ShapeDtypeStruct((1, 128), jnp.float32),
        ),
        in_specs=in_vmem(3 * count),
        out_specs=tuple(in_vmem(5)),
    )(*texts, *images, *pairs)

    if count == 2 and blocks & (blocks - 1) == 0:
        step = 1
        while step < blocks:
            moves = [(i, i ^ (2 * step + 1)) for i in range(blocks * count)]
            part = part + lax.ppermute(part, BOTH, moves)
            step *= 2
        loss = part[0, 0]
    else:
        loss = lax.psum(part[0, 0], BOTH) / count
    loss = loss / (2.0 * total * blocks)

    stats = (scores, row_lse, col_lse, pair_column)
    like = jax.ShapeDtypeStruct((rows, width), jnp.float32)

    def grad(kernel, pieces):
        return pl.pallas_call(
            functools.partial(kernel, count),
            out_shape=like,
            in_specs=in_vmem(count + 4),
            out_specs=pl.BlockSpec(memory_space=pltpu.VMEM),
            cost_estimate=pl.CostEstimate(
                flops=2 * rows * total * width, bytes_accessed=4 * rows * width, transcendentals=0
            ),
        )(*pieces, *stats)

    grad_text = grad(text_kernel, images)
    grad_image = grad(image_kernel, texts)
    return grad_text[None], grad_image[None], loss


def solution(mesh):
    placed = (P("blk", "grp", None), P("blk", "grp", None), P("blk", "grp"))
    return jax.shard_map(
        local,
        mesh=mesh,
        in_specs=placed,
        out_specs=(P("blk", "grp", None), P("blk", "grp", None), P()),
        check_vma=False,
    )
```

```python
import functools

import jax
import jax.numpy as jnp
from jax import lax
from jax.experimental import pallas as pl
from jax.experimental.pallas import tpu as pltpu
from jax.sharding import PartitionSpec as P


score_scale = 0.125
grad_scale = score_scale * 0.5
kernel_vmem = 24 << 20
BOTH = ("blk", "grp")


def column_of(row):
    n = row.shape[1]
    eye = lax.broadcasted_iota(jnp.int32, (n, n), 0) == lax.broadcasted_iota(jnp.int32, (n, n), 1)
    spread = jnp.where(eye, jnp.broadcast_to(row.astype(jnp.float32), (n, n)), 0.0)
    return jnp.sum(spread, axis=1, keepdims=True).astype(jnp.int32)


def square(text, image):
    both_last = (((1,), (1,)), ((), ()))
    return lax.dot_general(text, image, both_last, preferred_element_type=jnp.float32) * score_scale


def hit_of(count, pair_column, piece):
    rows = pair_column.shape[0]
    base = lax.rem(lax.axis_index("grp") + piece, count) * rows
    return pair_column - base == lax.broadcasted_iota(jnp.int32, (rows, rows), 1)


def own_kernel(text_hbm, image_hbm, pair_ref, text_ref, image_ref, pair_column_ref, score_ref, sems):
    loads = [
        pltpu.make_async_copy(text_hbm, text_ref, sems.at[0]),
        pltpu.make_async_copy(image_hbm, image_ref, sems.at[1]),
    ]
    for load in loads:
        load.start()
    pair_column_ref[...] = column_of(pair_ref[...])
    for load in loads:
        load.wait()
    score_ref[...] = square(text_ref[...], image_ref[...])


def stats_kernel(count, mean, *refs):
    refs = list(refs)

    def take(n):
        taken = refs[:n]
        del refs[:n]
        return taken

    texts, images, pairs = take(count), take(count), take(count - 1)
    own_score, own_pair = take(2)
    row_scores, col_scores = take(count - 1), take(count - 1)
    row_lses, col_lses, pair_columns = take(count), take(count), take(count - 1)
    (part_ref,) = take(1)
    rest = take((count - 1) ** 2)

    members = range(count)
    scores = {(0, 0): own_score}
    for k in range(1, count):
        scores[0, k] = row_scores[k - 1]
        scores[k, 0] = col_scores[k - 1]
    for a in range(1, count):
        for b in range(1, count):
            scores[a, b] = rest[(a - 1) * (count - 1) + b - 1]
    for b in members:
        for a in members:
            if a or b:
                scores[a, b][...] = square(texts[a][...], images[b][...])
    columns = [own_pair, *pair_columns]
    for k in range(1, count):
        pair_columns[k - 1][...] = column_of(pairs[k - 1][...])

    def added(values):
        return functools.reduce(jnp.add, values)

    def largest(values):
        return functools.reduce(jnp.maximum, values)

    def lse(line, axis):
        top = jnp.max(largest([s[...] for s in line]), axis=axis, keepdims=True)
        total = jnp.sum(added([jnp.exp(s[...] - top) for s in line]), axis=axis, keepdims=True)
        return top + jnp.log(total)

    for k in members:
        row_lses[k][...] = lse([scores[k, b] for b in members], 1)
        col_lses[k][...] = lse([scores[a, k] for a in members], 0)
    positive = 0.0
    for shift in members:
        positive += added(
            [
                jnp.where(
                    hit_of(count, columns[a][...], (a + shift) % count),
                    scores[a, (a + shift) % count][...],
                    0.0,
                )
                for a in members
            ]
        )
    part = (
        jnp.sum(added([r[...] for r in row_lses]), axis=0, keepdims=True)
        + jnp.sum(added([c[...] for c in col_lses]), axis=1, keepdims=True)
        - 2.0 * jnp.sum(jnp.sum(positive, axis=0, keepdims=True), axis=1, keepdims=True)
    )
    part_ref[...] = jnp.broadcast_to(part * mean, part_ref.shape)


def weight_of(score, row_lse, col_lse, hit):
    both = jnp.exp(score - row_lse) + jnp.exp(score - col_lse)
    return (both - jnp.where(hit, 2.0, 0.0)).astype(jnp.bfloat16)


def text_kernel(count, *refs):
    images, scores, cols = refs[:count], refs[count : 2 * count], refs[2 * count : 3 * count]
    row, pair, out_ref = refs[3 * count :]
    total = None
    for k in range(count):
        weight = weight_of(
            scores[k][...], row[...], cols[k][...], hit_of(count, pair[...], k)
        )
        term = jnp.dot(weight, images[k][...], preferred_element_type=jnp.float32)
        total = term if total is None else total + term
    out_ref[...] = total * grad_scale


def image_kernel(count, *refs):
    texts, scores, rows = refs[:count], refs[count : 2 * count], refs[2 * count : 3 * count]
    pairs = refs[3 * count : 4 * count]
    col, out_ref = refs[4 * count :]
    both_first = (((0,), (0,)), ((), ()))
    total = None
    for k in range(count):
        weight = weight_of(
            scores[k][...], rows[k][...], col[...], hit_of(count, pairs[k][...], 0)
        )
        term = lax.dot_general(
            weight, texts[k][...], both_first, preferred_element_type=jnp.float32
        )
        total = term if total is None else total + term
    out_ref[...] = total * grad_scale


def in_vmem(n):
    return [pl.BlockSpec(memory_space=pltpu.VMEM)] * n


def call(kernel, out_shape, args, flops, scratch=()):
    single = not isinstance(out_shape, tuple)
    return pl.pallas_call(
        kernel,
        out_shape=out_shape,
        in_specs=in_vmem(len(args)),
        out_specs=in_vmem(1)[0] if single else tuple(in_vmem(len(out_shape))),
        scratch_shapes=scratch,
        compiler_params=pltpu.CompilerParams(vmem_limit_bytes=kernel_vmem),
        cost_estimate=pl.CostEstimate(flops=flops, bytes_accessed=1, transcendentals=0),
    )(*[pltpu.with_memory_space_constraint(arg, pltpu.VMEM) for arg in args])


def local(text, image, pair_index):
    count = lax.axis_size("grp")
    blocks = lax.axis_size("blk")
    rows, width = text.shape[1:]
    total = rows * count
    dot_flops = 2 * rows * rows * width

    def others(value):
        return [
            lax.ppermute(value, "grp", [(i, (i - k) % count) for i in range(count)])
            for k in range(1, count)
        ]

    def piece(shape, dtype=jnp.float32):
        return pltpu.VMEM(shape, dtype)

    other_images = others(image[0])
    other_texts = others(text[0])
    other_pairs = others(pair_index)

    own_text, own_image, own_pair, own_score = pl.pallas_call(
        own_kernel,
        out_shape=(
            piece((rows, width), text.dtype),
            piece((rows, width), image.dtype),
            piece((rows, 1), jnp.int32),
            piece((rows, rows)),
        ),
        in_specs=[pl.BlockSpec(memory_space=pltpu.HBM)] * 2 + in_vmem(1),
        out_specs=tuple(in_vmem(4)),
        scratch_shapes=[pltpu.SemaphoreType.DMA((2,))],
        compiler_params=pltpu.CompilerParams(vmem_limit_bytes=kernel_vmem),
        cost_estimate=pl.CostEstimate(flops=20 * dot_flops, bytes_accessed=1, transcendentals=0),
    )(
        pltpu.with_memory_space_constraint(text[0], pltpu.HBM),
        pltpu.with_memory_space_constraint(image[0], pltpu.HBM),
        pltpu.with_memory_space_constraint(pair_index, pltpu.VMEM),
    )

    texts = [own_text, *other_texts]
    images = [own_image, *other_images]
    line = [piece((rows, rows))] * (count - 1)
    results = call(
        functools.partial(stats_kernel, count, 1.0 / (2.0 * total * blocks)),
        (
            *line,
            *line,
            *[piece((rows, 1))] * count,
            *[piece((1, rows))] * count,
            *[piece((rows, 1), jnp.int32)] * (count - 1),
            piece((1, 128)),
        ),
        [*texts, *images, *other_pairs, own_score, own_pair],
        dot_flops * count * count,
        [piece((rows, rows))] * (count - 1) ** 2,
    )
    results = list(results)
    row_scores = [own_score, *results[: count - 1]]
    col_scores = [own_score, *results[count - 1 : 2 * count - 2]]
    results = results[2 * count - 2 :]
    row_lses, col_lses = results[:count], results[count : 2 * count]
    pairs = [own_pair, *results[2 * count : -1]]
    part = results[-1]

    if count == 2 and blocks & (blocks - 1) == 0:
        step = 1
        while step < blocks:
            moves = [(i, i ^ (2 * step + 1)) for i in range(blocks * count)]
            part = part + lax.ppermute(part, BOTH, moves)
            step *= 2
        loss = part[0, 0]
    else:
        loss = lax.psum(part[0, 0], BOTH) / count

    like = jax.ShapeDtypeStruct((rows, width), jnp.float32)
    grad_text = call(
        functools.partial(text_kernel, count),
        like,
        [*images, *row_scores, *col_lses, row_lses[0], own_pair],
        4 * dot_flops * count,
    )
    grad_image = call(
        functools.partial(image_kernel, count),
        like,
        [*texts, *col_scores, *row_lses, *pairs, col_lses[0]],
        4 * dot_flops * count,
    )
    return grad_text[None], grad_image[None], loss


def solution(mesh):
    placed = (P("blk", "grp", None), P("blk", "grp", None), P("blk", "grp"))
    return jax.shard_map(
        local,
        mesh=mesh,
        in_specs=placed,
        out_specs=(P("blk", "grp", None), P("blk", "grp", None), P()),
        check_vma=False,
    )
```

```python
import functools

import jax
import jax.numpy as jnp
from jax import lax
from jax.experimental import pallas as pl
from jax.experimental.pallas import tpu as pltpu
from jax.sharding import PartitionSpec as P


score_scale = 0.125
log2_e = 1.4426950408889634
grad_scale = score_scale * 0.5
kernel_vmem = 24 << 20
grad_blocks = 4
BOTH = ("blk", "grp")


def column_of(row):
    n = row.shape[1]
    eye = lax.broadcasted_iota(jnp.int32, (n, n), 0) == lax.broadcasted_iota(jnp.int32, (n, n), 1)
    spread = jnp.where(eye, jnp.broadcast_to(row.astype(jnp.float32), (n, n)), 0.0)
    return jnp.sum(spread, axis=1, keepdims=True).astype(jnp.int32)


def square(text, image):
    both_last = (((1,), (1,)), ((), ()))
    return lax.dot_general(text, image, both_last, preferred_element_type=jnp.float32) * (
        score_scale * log2_e
    )


def hit_of(count, pair_column, piece):
    rows = pair_column.shape[0]
    base = lax.rem(lax.axis_index("grp") + piece, count) * rows
    return pair_column - base == lax.broadcasted_iota(jnp.int32, (rows, rows), 1)


def own_kernel(count, *refs):
    text_hbm, image_hbm, pair_hbm, text_ref, image_ref, pair_column_ref, hit_ref, score_ref = refs[:8]
    pair_ref, sems = refs[8:]
    loads = [
        pltpu.make_async_copy(text_hbm, text_ref, sems.at[0]),
        pltpu.make_async_copy(image_hbm, image_ref, sems.at[1]),
        pltpu.make_async_copy(pair_hbm, pair_ref, sems.at[2]),
    ]
    for load in loads:
        load.start()
    loads[2].wait()
    pair_column_ref[...] = column_of(pair_ref[...])
    for load in loads[:2]:
        load.wait()
    score_ref[...] = square(text_ref[...], image_ref[...])
    hit_ref[...] = jnp.sum(hits_of(count, pair_column_ref, 0, score_ref), axis=1, keepdims=True)


def added(values):
    return functools.reduce(jnp.add, values)


def lse(line, axis):
    top = functools.reduce(jnp.maximum, [s[...] for s in line])
    top = jnp.max(top, axis=axis, keepdims=True)
    total = jnp.sum(added([jnp.exp2(s[...] - top) for s in line]), axis=axis, keepdims=True)
    return top + jnp.log(total) * log2_e


def hits_of(count, pair_column, piece, score):
    return jnp.where(hit_of(count, pair_column[...], piece), score[...], 0.0)


def stats_kernel(count, mean, *refs):
    refs = list(refs)

    def take(n):
        taken = refs[:n]
        del refs[:n]
        return taken

    texts, images, pairs = take(count), take(count), take(count - 1)
    own_pair, own_hit, own_score = take(3)
    col_scores, row_scores = take(count - 1), take(count - 1)
    row_lses, col_lses, pair_columns = take(count), take(count), take(count - 1)
    (part_ref,) = take(1)
    rest = take((count - 1) ** 2)

    members = range(count)
    rows = own_score.shape[0]
    columns = [own_pair, *pair_columns]
    for k in range(1, count):
        pair_columns[k - 1][...] = column_of(pairs[k - 1][...])
    scores = {(0, 0): own_score}
    for k in range(1, count):
        scores[k, 0] = col_scores[k - 1]
        scores[0, k] = row_scores[k - 1]
        for a in range(1, count):
            scores[a, k] = rest[(a - 1) * (count - 1) + k - 1]
    for b in members:
        line = [a for a in members if a or b]
        product = square(jnp.concatenate([texts[a][...] for a in line], axis=0), images[b][...])
        for n, a in enumerate(line):
            scores[a, b][...] = product[n * rows : (n + 1) * rows]

    for k in members:
        col_lses[k][...] = lse([scores[a, k] for a in members], 0)
        row_lses[k][...] = lse([scores[k, b] for b in members], 1)
    hits = []
    for a in members:
        pieces = [hits_of(count, columns[a], b, scores[a, b]) for b in members if a or b]
        hits.append(jnp.sum(added(pieces), axis=1, keepdims=True))
    hits[0] += own_hit[...]
    line = added([r[...] - 2.0 * h for r, h in zip(row_lses, hits)])
    cols = added([c[...] for c in col_lses])
    part = jnp.sum(line, axis=0, keepdims=True) + jnp.sum(cols, axis=1, keepdims=True)
    part_ref[...] = jnp.broadcast_to(part * mean, part_ref.shape)


def weight_of(score, row_lse, col_lse, hit):
    both = jnp.exp2(score - row_lse) + jnp.exp2(score - col_lse)
    return (both - jnp.where(hit, 2.0, 0.0)).astype(jnp.bfloat16)


def write_out(weights, pieces, dims, out_hbm, block_ref, sems):
    step = block_ref.shape[1] // sems.shape[0]
    stores = []
    for n in range(sems.shape[0]):
        at = slice(n * step, (n + 1) * step)
        terms = [
            lax.dot_general(w, p[:, at], (dims, ((), ())), preferred_element_type=jnp.float32)
            for w, p in zip(weights, pieces)
        ]
        block_ref[:, at] = added(terms) * grad_scale
        store = pltpu.make_async_copy(block_ref.at[:, at], out_hbm.at[:, at], sems.at[n])
        store.start()
        stores.append(store)
    for store in stores:
        store.wait()


def text_kernel(count, *refs):
    images, scores, cols = refs[:count], refs[count : 2 * count], refs[2 * count : 3 * count]
    row, pair, out_hbm, block_ref, sems = refs[3 * count :]
    weights = [
        weight_of(scores[k][...], row[...], cols[k][...], hit_of(count, pair[...], k))
        for k in range(count)
    ]
    write_out(weights, images, ((1,), (0,)), out_hbm, block_ref, sems)


def image_kernel(count, *refs):
    texts, scores, rows = refs[:count], refs[count : 2 * count], refs[2 * count : 3 * count]
    pairs = refs[3 * count : 4 * count]
    col, out_hbm, block_ref, sems = refs[4 * count :]
    weights = [
        weight_of(scores[k][...], rows[k][...], col[...], hit_of(count, pairs[k][...], 0))
        for k in range(count)
    ]
    write_out(weights, texts, ((0,), (0,)), out_hbm, block_ref, sems)


def in_vmem(n):
    return [pl.BlockSpec(memory_space=pltpu.VMEM)] * n


def call(kernel, out_shape, args, flops, scratch=(), out_space=pltpu.VMEM):
    single = not isinstance(out_shape, tuple)
    place = pl.BlockSpec(memory_space=out_space)
    return pl.pallas_call(
        kernel,
        out_shape=out_shape,
        in_specs=in_vmem(len(args)),
        out_specs=place if single else (place,) * len(out_shape),
        scratch_shapes=scratch,
        compiler_params=pltpu.CompilerParams(vmem_limit_bytes=kernel_vmem),
        cost_estimate=pl.CostEstimate(flops=flops, bytes_accessed=1, transcendentals=0),
    )(*[pltpu.with_memory_space_constraint(arg, pltpu.VMEM) for arg in args])


def rounds(blocks):
    bits = [1 << k for k in range(blocks.bit_length() - 1)]
    if len(bits) < 3:
        return [(bit,) for bit in bits]
    *near, third, second, first = bits
    return [(first | second,), (second | third, third, second), *[(bit,) for bit in near]]


def local(text, image, pair_index):
    count = lax.axis_size("grp")
    blocks = lax.axis_size("blk")
    rows, width = text.shape[1:]
    total = rows * count
    dot_flops = 2 * rows * rows * width

    def others(value):
        return [
            lax.ppermute(value, "grp", [(i, (i - k) % count) for i in range(count)])
            for k in range(1, count)
        ]

    def piece(shape, dtype=jnp.float32):
        return pltpu.VMEM(shape, dtype)

    other_pairs = others(pair_index)
    other_texts = others(text[0])
    other_images = others(image[0])

    own_text, own_image, own_pair, own_hit, own_score = pl.pallas_call(
        functools.partial(own_kernel, count),
        out_shape=(
            piece((rows, width), text.dtype),
            piece((rows, width), image.dtype),
            piece((rows, 1), jnp.int32),
            piece((rows, 1)),
            piece((rows, rows)),
        ),
        in_specs=[pl.BlockSpec(memory_space=pltpu.HBM)] * 3,
        out_specs=tuple(in_vmem(5)),
        scratch_shapes=[piece((1, rows), jnp.int32), pltpu.SemaphoreType.DMA((3,))],
        compiler_params=pltpu.CompilerParams(vmem_limit_bytes=kernel_vmem),
        cost_estimate=pl.CostEstimate(flops=4 * dot_flops, bytes_accessed=1, transcendentals=0),
    )(
        pltpu.with_memory_space_constraint(text[0], pltpu.HBM),
        pltpu.with_memory_space_constraint(image[0], pltpu.HBM),
        pltpu.with_memory_space_constraint(pair_index, pltpu.HBM),
    )

    texts = [own_text, *other_texts]
    images = [own_image, *other_images]
    line = [piece((rows, rows))] * (count - 1)
    results = call(
        functools.partial(stats_kernel, count, 1.0 / (2.0 * log2_e * total * blocks)),
        (
            *line,
            *line,
            *[piece((rows, 1))] * count,
            *[piece((1, rows))] * count,
            *[piece((rows, 1), jnp.int32)] * (count - 1),
            piece((1, 128)),
        ),
        [*texts, *images, *other_pairs, own_pair, own_hit, own_score],
        dot_flops * count * count,
        [piece((rows, rows))] * (count - 1) ** 2,
    )
    results = list(results)
    col_scores = [own_score, *results[: count - 1]]
    row_scores = [own_score, *results[count - 1 : 2 * count - 2]]
    results = results[2 * count - 2 :]
    row_lses, col_lses = results[:count], results[count : 2 * count]
    pairs = [own_pair, *results[2 * count : -1]]
    part = results[-1]

    if count == 2 and blocks & (blocks - 1) == 0:
        for flips in rounds(blocks):
            got = []
            for flip in flips:
                moves = [(i, i ^ (2 * flip + 1)) for i in range(blocks * count)]
                got.append(lax.ppermute(part, BOTH, moves))
            part = part + got[0] if len(got) == 1 else (part + got[1]) + (got[0] + got[2])
        loss = part[0, 0]
    else:
        loss = lax.psum(part[0, 0], BOTH) / count

    like = jax.ShapeDtypeStruct((rows, width), jnp.float32)
    stage = [piece((rows, width)), pltpu.SemaphoreType.DMA((grad_blocks,))]
    grad_text = call(
        functools.partial(text_kernel, count),
        like,
        [*images, *row_scores, *col_lses, row_lses[0], own_pair],
        4 * dot_flops * count,
        stage,
        pltpu.HBM,
    )
    grad_image = call(
        functools.partial(image_kernel, count),
        like,
        [*texts, *col_scores, *row_lses, *pairs, col_lses[0]],
        4 * dot_flops * count,
        stage,
        pltpu.HBM,
    )
    return grad_text[None], grad_image[None], loss


def solution(mesh):
    placed = (P("blk", "grp", None), P("blk", "grp", None), P("blk", "grp"))
    return jax.shard_map(
        local,
        mesh=mesh,
        in_specs=placed,
        out_specs=(P("blk", "grp", None), P("blk", "grp", None), P()),
        check_vma=False,
    )
```

```python
import functools

import jax
import jax.numpy as jnp
from jax import lax
from jax.experimental import pallas as pl
from jax.experimental.pallas import tpu as pltpu
from jax.sharding import PartitionSpec as P


score_scale = 0.125
log2_e = 1.4426950408889634
grad_scale = score_scale * 0.5
kernel_vmem = 24 << 20
grad_blocks = 4
BOTH = ("blk", "grp")


def column_of(row):
    n = row.shape[1]
    eye = lax.broadcasted_iota(jnp.int32, (n, n), 0) == lax.broadcasted_iota(jnp.int32, (n, n), 1)
    spread = jnp.where(eye, jnp.broadcast_to(row.astype(jnp.float32), (n, n)), 0.0)
    return jnp.sum(spread, axis=1, keepdims=True).astype(jnp.int32)


def square(text, image):
    both_last = (((1,), (1,)), ((), ()))
    return lax.dot_general(text, image, both_last, preferred_element_type=jnp.float32) * (
        score_scale * log2_e
    )


def hit_of(count, pair_column, piece):
    rows = pair_column.shape[0]
    base = lax.rem(lax.axis_index("grp") + piece, count) * rows
    return pair_column - base == lax.broadcasted_iota(jnp.int32, (rows, rows), 1)


def own_kernel(count, *refs):
    text_hbm, image_hbm, pair_hbm, text_ref, image_ref, pair_column_ref, hit_ref, score_ref = refs[:8]
    pair_ref, sems = refs[8:]
    loads = [
        pltpu.make_async_copy(text_hbm, text_ref, sems.at[0]),
        pltpu.make_async_copy(image_hbm, image_ref, sems.at[1]),
        pltpu.make_async_copy(pair_hbm, pair_ref, sems.at[2]),
    ]
    for load in loads:
        load.start()
    loads[2].wait()
    pair_column_ref[...] = column_of(pair_ref[...])
    for load in loads[:2]:
        load.wait()
    score_ref[...] = square(text_ref[...], image_ref[...])
    hit_ref[...] = jnp.sum(hits_of(count, pair_column_ref, 0, score_ref), axis=0, keepdims=True)


def added(values):
    return functools.reduce(jnp.add, values)


def lse(line, axis):
    top = functools.reduce(jnp.maximum, [s[...] for s in line])
    top = jnp.max(top, axis=axis, keepdims=True)
    total = jnp.sum(added([jnp.exp2(s[...] - top) for s in line]), axis=axis, keepdims=True)
    return top + jnp.log(total) * log2_e


def hits_of(count, pair_column, piece, score):
    return jnp.where(hit_of(count, pair_column[...], piece), score[...], 0.0)


def stats_kernel(count, mean, *refs):
    refs = list(refs)

    def take(n):
        taken = refs[:n]
        del refs[:n]
        return taken

    texts, images, pairs = take(count), take(count), take(count - 1)
    own_pair, own_hit, own_score = take(3)
    col_scores, row_scores = take(count - 1), take(count - 1)
    row_lses, col_lses, pair_columns = take(count), take(count), take(count - 1)
    (part_ref,) = take(1)
    rest = take((count - 1) ** 2)

    members = range(count)
    rows = own_score.shape[0]
    columns = [own_pair, *pair_columns]
    for k in range(1, count):
        pair_columns[k - 1][...] = column_of(pairs[k - 1][...])
    scores = {(0, 0): own_score}
    for k in range(1, count):
        scores[k, 0] = col_scores[k - 1]
        scores[0, k] = row_scores[k - 1]
        for a in range(1, count):
            scores[a, k] = rest[(a - 1) * (count - 1) + k - 1]
    for b in members:
        line = [a for a in members if a or b]
        product = square(jnp.concatenate([texts[a][...] for a in line], axis=0), images[b][...])
        for n, a in enumerate(line):
            scores[a, b][...] = product[n * rows : (n + 1) * rows]

    for k in members:
        col_lses[k][...] = lse([scores[a, k] for a in members], 0)
        row_lses[k][...] = lse([scores[k, b] for b in members], 1)
    hits = []
    for b in members:
        pieces = [hits_of(count, columns[a], b, scores[a, b]) for a in members if a or b]
        hits.append(jnp.sum(added(pieces), axis=0, keepdims=True))
    hits[0] += own_hit[...]
    cols = added([c[...] - 2.0 * h for c, h in zip(col_lses, hits)])
    line = jnp.sum(added([r[...] for r in row_lses]), axis=0, keepdims=True)
    part = line + jnp.sum(cols, axis=1, keepdims=True)
    part_ref[...] = jnp.broadcast_to(part * mean, part_ref.shape)


def weight_of(score, row_lse, col_lse, hit):
    both = jnp.exp2(score - row_lse) + jnp.exp2(score - col_lse)
    return (both - jnp.where(hit, 2.0, 0.0)).astype(jnp.bfloat16)


def write_out(weights, pieces, dims, out_hbm, block_ref, sems):
    step = block_ref.shape[1] // sems.shape[0]
    stores = []
    for n in range(sems.shape[0]):
        at = slice(n * step, (n + 1) * step)
        terms = [
            lax.dot_general(w, p[:, at], (dims, ((), ())), preferred_element_type=jnp.float32)
            for w, p in zip(weights, pieces)
        ]
        block_ref[:, at] = added(terms) * grad_scale
        store = pltpu.make_async_copy(block_ref.at[:, at], out_hbm.at[:, at], sems.at[n])
        store.start()
        stores.append(store)
    for store in stores:
        store.wait()


def text_kernel(count, *refs):
    images, scores, cols = refs[:count], refs[count : 2 * count], refs[2 * count : 3 * count]
    row, pair, out_hbm, block_ref, sems = refs[3 * count :]
    weights = [
        weight_of(scores[k][...], row[...], cols[k][...], hit_of(count, pair[...], k))
        for k in range(count)
    ]
    write_out(weights, images, ((1,), (0,)), out_hbm, block_ref, sems)


def image_kernel(count, *refs):
    texts, scores, rows = refs[:count], refs[count : 2 * count], refs[2 * count : 3 * count]
    pairs = refs[3 * count : 4 * count]
    col, out_hbm, block_ref, sems = refs[4 * count :]
    weights = [
        weight_of(scores[k][...], rows[k][...], col[...], hit_of(count, pairs[k][...], 0))
        for k in range(count)
    ]
    write_out(weights, texts, ((0,), (0,)), out_hbm, block_ref, sems)


def in_vmem(n):
    return [pl.BlockSpec(memory_space=pltpu.VMEM)] * n


def call(kernel, out_shape, args, flops, scratch=(), out_space=pltpu.VMEM):
    single = not isinstance(out_shape, tuple)
    place = pl.BlockSpec(memory_space=out_space)
    return pl.pallas_call(
        kernel,
        out_shape=out_shape,
        in_specs=in_vmem(len(args)),
        out_specs=place if single else (place,) * len(out_shape),
        scratch_shapes=scratch,
        compiler_params=pltpu.CompilerParams(vmem_limit_bytes=kernel_vmem),
        cost_estimate=pl.CostEstimate(flops=flops, bytes_accessed=1, transcendentals=0),
    )(*[pltpu.with_memory_space_constraint(arg, pltpu.VMEM) for arg in args])


def rounds(blocks):
    bits = [1 << k for k in range(blocks.bit_length() - 1)]
    if len(bits) < 3:
        return [(bit,) for bit in bits]
    *near, third, second, first = bits
    return [(first | second,), (second | third, third, second), *[(bit,) for bit in near]]


def local(text, image, pair_index):
    count = lax.axis_size("grp")
    blocks = lax.axis_size("blk")
    rows, width = text.shape[1:]
    total = rows * count
    dot_flops = 2 * rows * rows * width

    def others(value):
        return [
            lax.ppermute(value, "grp", [(i, (i - k) % count) for i in range(count)])
            for k in range(1, count)
        ]

    def piece(shape, dtype=jnp.float32):
        return pltpu.VMEM(shape, dtype)

    other_pairs = others(pair_index)
    other_texts = others(text[0])
    other_images = others(image[0])

    own_text, own_image, own_pair, own_hit, own_score = pl.pallas_call(
        functools.partial(own_kernel, count),
        out_shape=(
            piece((rows, width), text.dtype),
            piece((rows, width), image.dtype),
            piece((rows, 1), jnp.int32),
            piece((1, rows)),
            piece((rows, rows)),
        ),
        in_specs=[pl.BlockSpec(memory_space=pltpu.HBM)] * 3,
        out_specs=tuple(in_vmem(5)),
        scratch_shapes=[piece((1, rows), jnp.int32), pltpu.SemaphoreType.DMA((3,))],
        compiler_params=pltpu.CompilerParams(vmem_limit_bytes=kernel_vmem),
        cost_estimate=pl.CostEstimate(flops=4 * dot_flops, bytes_accessed=1, transcendentals=0),
    )(
        pltpu.with_memory_space_constraint(text[0], pltpu.HBM),
        pltpu.with_memory_space_constraint(image[0], pltpu.HBM),
        pltpu.with_memory_space_constraint(pair_index, pltpu.HBM),
    )

    texts = [own_text, *other_texts]
    images = [own_image, *other_images]
    line = [piece((rows, rows))] * (count - 1)
    results = call(
        functools.partial(stats_kernel, count, 1.0 / (2.0 * log2_e * total * blocks)),
        (
            *line,
            *line,
            *[piece((rows, 1))] * count,
            *[piece((1, rows))] * count,
            *[piece((rows, 1), jnp.int32)] * (count - 1),
            piece((1, 128)),
        ),
        [*texts, *images, *other_pairs, own_pair, own_hit, own_score],
        dot_flops * count * count,
        [piece((rows, rows))] * (count - 1) ** 2,
    )
    results = list(results)
    col_scores = [own_score, *results[: count - 1]]
    row_scores = [own_score, *results[count - 1 : 2 * count - 2]]
    results = results[2 * count - 2 :]
    row_lses, col_lses = results[:count], results[count : 2 * count]
    pairs = [own_pair, *results[2 * count : -1]]
    part = results[-1]

    if count == 2 and blocks & (blocks - 1) == 0:
        for flips in rounds(blocks):
            got = []
            for flip in flips:
                moves = [(i, i ^ (2 * flip + 1)) for i in range(blocks * count)]
                got.append(lax.ppermute(part, BOTH, moves))
            part = part + got[0] if len(got) == 1 else (part + got[1]) + (got[0] + got[2])
        loss = part[0, 0]
    else:
        loss = lax.psum(part[0, 0], BOTH) / count

    like = jax.ShapeDtypeStruct((rows, width), jnp.float32)
    stage = [piece((rows, width)), pltpu.SemaphoreType.DMA((grad_blocks,))]
    grad_text = call(
        functools.partial(text_kernel, count),
        like,
        [*images, *row_scores, *col_lses, row_lses[0], own_pair],
        4 * dot_flops * count,
        stage,
        pltpu.HBM,
    )
    grad_image = call(
        functools.partial(image_kernel, count),
        like,
        [*texts, *col_scores, *row_lses, *pairs, col_lses[0]],
        4 * dot_flops * count,
        stage,
        pltpu.HBM,
    )
    return grad_text[None], grad_image[None], loss


def solution(mesh):
    placed = (P("blk", "grp", None), P("blk", "grp", None), P("blk", "grp"))
    return jax.shard_map(
        local,
        mesh=mesh,
        in_specs=placed,
        out_specs=(P("blk", "grp", None), P("blk", "grp", None), P()),
        check_vma=False,
    )
```

```python
import functools

import jax
import jax.numpy as jnp
from jax import lax
from jax.experimental import pallas as pl
from jax.experimental.pallas import tpu as pltpu
from jax.sharding import PartitionSpec as P


score_scale = 0.125
log2_e = 1.4426950408889634
grad_scale = score_scale * 0.5
kernel_vmem = 24 << 20
grad_blocks = 4
BOTH = ("blk", "grp")


def column_of(row):
    n = row.shape[1]
    eye = lax.broadcasted_iota(jnp.int32, (n, n), 0) == lax.broadcasted_iota(jnp.int32, (n, n), 1)
    spread = jnp.where(eye, jnp.broadcast_to(row.astype(jnp.float32), (n, n)), 0.0)
    return jnp.sum(spread, axis=1, keepdims=True)


def square(text, image):
    both_last = (((1,), (1,)), ((), ()))
    return lax.dot_general(text, image, both_last, preferred_element_type=jnp.float32) * (
        score_scale * log2_e
    )


def hit_of(count, pair_column, piece):
    rows = pair_column.shape[0]
    base = lax.rem(lax.axis_index("grp") + piece, count) * rows
    ids = lax.broadcasted_iota(jnp.int32, (1, rows), 1) + base
    return pair_column == ids.astype(jnp.float32)


def own_kernel(count, *refs):
    text_hbm, image_hbm, pair_hbm, text_ref, image_ref, pair_column_ref, hit_ref, score_ref = refs[:8]
    pair_ref, sems = refs[8:]
    loads = [
        pltpu.make_async_copy(text_hbm, text_ref, sems.at[0]),
        pltpu.make_async_copy(image_hbm, image_ref, sems.at[1]),
        pltpu.make_async_copy(pair_hbm, pair_ref, sems.at[2]),
    ]
    for load in loads:
        load.start()
    loads[2].wait()
    pair_column_ref[...] = column_of(pair_ref[...])
    for load in loads[:2]:
        load.wait()
    score_ref[...] = square(text_ref[...], image_ref[...])
    hit_ref[...] = jnp.sum(hits_of(count, pair_column_ref, 0, score_ref), axis=0, keepdims=True)


def added(values):
    return functools.reduce(jnp.add, values)


def lse(line, axis):
    top = functools.reduce(jnp.maximum, [s[...] for s in line])
    top = jnp.max(top, axis=axis, keepdims=True)
    total = jnp.sum(added([jnp.exp2(s[...] - top) for s in line]), axis=axis, keepdims=True)
    return top + jnp.log(total) * log2_e


def hits_of(count, pair_column, piece, score):
    return jnp.where(hit_of(count, pair_column[...], piece), score[...], 0.0)


def stats_kernel(count, mean, *refs):
    refs = list(refs)

    def take(n):
        taken = refs[:n]
        del refs[:n]
        return taken

    texts, images, pairs = take(count), take(count), take(count - 1)
    own_pair, own_hit, own_score = take(3)
    col_scores, row_scores = take(count - 1), take(count - 1)
    row_lses, col_lses, pair_columns = take(count), take(count), take(count - 1)
    (part_ref,) = take(1)
    rest = take((count - 1) ** 2)

    members = range(count)
    rows = own_score.shape[0]
    columns = [own_pair, *pair_columns]
    for k in range(1, count):
        pair_columns[k - 1][...] = column_of(pairs[k - 1][...])
    scores = {(0, 0): own_score}
    for k in range(1, count):
        scores[k, 0] = col_scores[k - 1]
        scores[0, k] = row_scores[k - 1]
        for a in range(1, count):
            scores[a, k] = rest[(a - 1) * (count - 1) + k - 1]
    for b in members:
        line = [a for a in members if a or b]
        product = square(jnp.concatenate([texts[a][...] for a in line], axis=0), images[b][...])
        for n, a in enumerate(line):
            scores[a, b][...] = product[n * rows : (n + 1) * rows]

    for k in members:
        col_lses[k][...] = lse([scores[a, k] for a in members], 0)
        row_lses[k][...] = lse([scores[k, b] for b in members], 1)
    hits = []
    for b in members:
        pieces = [hits_of(count, columns[a], b, scores[a, b]) for a in members if a or b]
        hits.append(jnp.sum(added(pieces), axis=0, keepdims=True))
    hits[0] += own_hit[...]
    cols = added([c[...] - 2.0 * h for c, h in zip(col_lses, hits)])
    line = jnp.sum(added([r[...] for r in row_lses]), axis=0, keepdims=True)
    part = line + jnp.sum(cols, axis=1, keepdims=True)
    part_ref[...] = jnp.broadcast_to(part * mean, part_ref.shape)


def weight_of(score, row_lse, col_lse, hit):
    both = jnp.exp2(score - row_lse) + jnp.exp2(score - col_lse)
    return (both - jnp.where(hit, 2.0, 0.0)).astype(jnp.bfloat16)


def write_out(weights, pieces, dims, out_hbm, block_ref, sems):
    step = block_ref.shape[1] // sems.shape[0]
    stores = []
    for n in range(sems.shape[0]):
        at = slice(n * step, (n + 1) * step)
        terms = [
            lax.dot_general(w, p[:, at], (dims, ((), ())), preferred_element_type=jnp.float32)
            for w, p in zip(weights, pieces)
        ]
        block_ref[:, at] = added(terms) * grad_scale
        store = pltpu.make_async_copy(block_ref.at[:, at], out_hbm.at[:, at], sems.at[n])
        store.start()
        stores.append(store)
    for store in stores:
        store.wait()


def text_kernel(count, *refs):
    images, scores, cols = refs[:count], refs[count : 2 * count], refs[2 * count : 3 * count]
    row, pair, out_hbm, block_ref, sems = refs[3 * count :]
    weights = [
        weight_of(scores[k][...], row[...], cols[k][...], hit_of(count, pair[...], k))
        for k in range(count)
    ]
    write_out(weights, images, ((1,), (0,)), out_hbm, block_ref, sems)


def image_kernel(count, *refs):
    texts, scores, rows = refs[:count], refs[count : 2 * count], refs[2 * count : 3 * count]
    pairs = refs[3 * count : 4 * count]
    col, out_hbm, block_ref, sems = refs[4 * count :]
    weights = [
        weight_of(scores[k][...], rows[k][...], col[...], hit_of(count, pairs[k][...], 0))
        for k in range(count)
    ]
    write_out(weights, texts, ((0,), (0,)), out_hbm, block_ref, sems)


def in_vmem(n):
    return [pl.BlockSpec(memory_space=pltpu.VMEM)] * n


def call(kernel, out_shape, args, flops, scratch=(), out_space=pltpu.VMEM):
    single = not isinstance(out_shape, tuple)
    place = pl.BlockSpec(memory_space=out_space)
    return pl.pallas_call(
        kernel,
        out_shape=out_shape,
        in_specs=in_vmem(len(args)),
        out_specs=place if single else (place,) * len(out_shape),
        scratch_shapes=scratch,
        compiler_params=pltpu.CompilerParams(vmem_limit_bytes=kernel_vmem),
        cost_estimate=pl.CostEstimate(flops=flops, bytes_accessed=1, transcendentals=0),
    )(*[pltpu.with_memory_space_constraint(arg, pltpu.VMEM) for arg in args])


def rounds(blocks):
    bits = [1 << k for k in range(blocks.bit_length() - 1)]
    if len(bits) < 3:
        return [(bit,) for bit in bits]
    *near, third, second, first = bits
    return [(first | second,), (second | third, third, second), *[(bit,) for bit in near]]


def local(text, image, pair_index):
    count = lax.axis_size("grp")
    blocks = lax.axis_size("blk")
    rows, width = text.shape[1:]
    total = rows * count
    dot_flops = 2 * rows * rows * width

    def others(value):
        return [
            lax.ppermute(value, "grp", [(i, (i - k) % count) for i in range(count)])
            for k in range(1, count)
        ]

    def piece(shape, dtype=jnp.float32):
        return pltpu.VMEM(shape, dtype)

    other_pairs = others(pair_index)
    other_texts = others(text[0])
    other_images = others(image[0])

    own_text, own_image, own_pair, own_hit, own_score = pl.pallas_call(
        functools.partial(own_kernel, count),
        out_shape=(
            piece((rows, width), text.dtype),
            piece((rows, width), image.dtype),
            piece((rows, 1)),
            piece((1, rows)),
            piece((rows, rows)),
        ),
        in_specs=[pl.BlockSpec(memory_space=pltpu.HBM)] * 3,
        out_specs=tuple(in_vmem(5)),
        scratch_shapes=[piece((1, rows), jnp.int32), pltpu.SemaphoreType.DMA((3,))],
        compiler_params=pltpu.CompilerParams(vmem_limit_bytes=kernel_vmem),
        cost_estimate=pl.CostEstimate(flops=4 * dot_flops, bytes_accessed=1, transcendentals=0),
    )(
        pltpu.with_memory_space_constraint(text[0], pltpu.HBM),
        pltpu.with_memory_space_constraint(image[0], pltpu.HBM),
        pltpu.with_memory_space_constraint(pair_index, pltpu.HBM),
    )

    texts = [own_text, *other_texts]
    images = [own_image, *other_images]
    line = [piece((rows, rows))] * (count - 1)
    results = call(
        functools.partial(stats_kernel, count, 1.0 / (2.0 * log2_e * total * blocks)),
        (
            *line,
            *line,
            *[piece((rows, 1))] * count,
            *[piece((1, rows))] * count,
            *[piece((rows, 1))] * (count - 1),
            piece((1, 128)),
        ),
        [*texts, *images, *other_pairs, own_pair, own_hit, own_score],
        dot_flops * count * count,
        [piece((rows, rows))] * (count - 1) ** 2,
    )
    results = list(results)
    col_scores = [own_score, *results[: count - 1]]
    row_scores = [own_score, *results[count - 1 : 2 * count - 2]]
    results = results[2 * count - 2 :]
    row_lses, col_lses = results[:count], results[count : 2 * count]
    pairs = [own_pair, *results[2 * count : -1]]
    part = results[-1]

    if count == 2 and blocks & (blocks - 1) == 0:
        for flips in rounds(blocks):
            got = []
            for flip in flips:
                moves = [(i, i ^ (2 * flip + 1)) for i in range(blocks * count)]
                got.append(lax.ppermute(part, BOTH, moves))
            part = part + got[0] if len(got) == 1 else (part + got[1]) + (got[0] + got[2])
        loss = part[0, 0]
    else:
        loss = lax.psum(part[0, 0], BOTH) / count

    like = jax.ShapeDtypeStruct((rows, width), jnp.float32)
    stage = [piece((rows, width)), pltpu.SemaphoreType.DMA((grad_blocks,))]
    grad_text = call(
        functools.partial(text_kernel, count),
        like,
        [*images, *row_scores, *col_lses, row_lses[0], own_pair],
        4 * dot_flops * count,
        stage,
        pltpu.HBM,
    )
    grad_image = call(
        functools.partial(image_kernel, count),
        like,
        [*texts, *col_scores, *row_lses, *pairs, col_lses[0]],
        4 * dot_flops * count,
        stage,
        pltpu.HBM,
    )
    return grad_text[None], grad_image[None], loss


def solution(mesh):
    placed = (P("blk", "grp", None), P("blk", "grp", None), P("blk", "grp"))
    return jax.shard_map(
        local,
        mesh=mesh,
        in_specs=placed,
        out_specs=(P("blk", "grp", None), P("blk", "grp", None), P()),
        check_vma=False,
    )
```
